32 devices in a mesh: seq: 16 (over z, x, core), chan: 2 (over y).
Axes of the slice: x: 2, y: 2, z: 4, core: 2. Of those that a mesh axis runs over, the one named last changes fastest.
Arguments:
- signal: bfloat16 [524288, 256], P('seq', 'chan'), parts along dimension 1, may hold values from -6 to 6
- gate_values: bfloat16 [524288, 256], P('seq', 'chan'), parts along dimension 1, may hold values from -4 to 4
- skip_gain: float32 [256], P('chan'), parts along dimension 0, may hold values from 0.25 to 2
- filter_spectrum: bfloat16 [2, 512, 1024, 256], P(None, 'seq', None, 'chan'), parts along dimension 3, may hold values from -4 to 4, as said below
Outputs:
- gated_output: bfloat16 [524288, 256], P('seq', 'chan'), parts along dimension 1
The draws below stay inside these ranges and needn't reach their ends.
There are 2 independent parts, one for each index of `chan`. The reference program is written for one: setup_inputs(seed, part) draws one part's arguments, and reference() takes and returns one part's arrays. A program takes and returns all parts, laid end to end along the dimension named above; each array names one. Nothing has to cross between parts.
Inputs may be any that keep to these rules, and one draw needn't show every extreme that they name: `filter_spectrum`: the spectrum of a real filter: the complex entry at frequency k equals the conjugate of the entry at frequency (524288 - k) mod 524288.
All inputs are finite; a program needn't handle non-finite values.
Results may differ from the reference program's by a relative error of at most 0.0085.
Values may be sent and summed in bfloat16 or wider, within the bound.
No kernel may reach another device: no remote copies, remote signals or barrier semaphores. Data moves between devices by JAX's collectives and lax.ppermute only.
A program may use at most 256 MiB of HBM per device.

```python
import math
import jax
import jax.numpy as jnp
from jax import lax

OUTER = 1024
INNER = 512
CH = 128
SEQ = 524288


def draw_filter_spectrum(key, part):
    length = INNER * OUTER
    first_key = jax.random.fold_in(key, 11)
    base = jax.random.normal(first_key, (2, length, CH), jnp.float32)
    mirror = jnp.roll(jnp.flip(base, axis=1), 1, axis=1)
    real_part = (base[0] + mirror[0]) * 0.7071
    imag_part = (base[1] - mirror[1]) * 0.7071
    both = jnp.clip(jnp.stack([real_part, imag_part]), -4.0, 4.0)
    return both.reshape(2, INNER, OUTER, CH).astype(jnp.bfloat16)


def level_of(rng, extent, split, smallest, top_value):
    factor_of = 1.0
    for axis_at, blocks in split:
        heights = jax.random.uniform(jax.random.fold_in(jax.random.fold_in(rng, 6), axis_at), (blocks,), jnp.float32, smallest / len(split), top_value / len(split))
        factor_of = factor_of * jnp.repeat(jnp.exp(heights), extent[axis_at] // blocks).reshape((-1,) + (1,) * (len(extent) - 1 - axis_at))
    return factor_of


def centred(rng, extent, scale, limit, cuts=(), held_as=jnp.bfloat16):
    level = level_of(rng, extent, cuts, -0.22, 0.18) if cuts else 1.0
    values = jax.random.normal(rng, extent, jnp.float32) * scale * level
    return jnp.minimum(jnp.maximum(values, -limit), limit).astype(held_as)


def setup_inputs(seed: int = 0, part: int = 0) -> dict:
    keys = jax.random.split(jax.random.key(seed), 5)
    part_keys = jax.random.split(jax.random.fold_in(keys[4], part), 5)
    signal = centred(part_keys[0], (SEQ, CH), 1.0, 6.0, ((0, 16),))
    gate_values = centred(part_keys[1], (SEQ, CH), 1.0, 4.0, ((0, 16),))
    skip_gain = jnp.clip(jnp.exp(jax.random.uniform(part_keys[2], (CH,), jnp.float32, math.log(0.25), math.log(2.0))), 0.25, 2.0)
    filter_spectrum = draw_filter_spectrum(jax.random.fold_in(jax.random.fold_in(keys[4], part), 71), part)
    return {"signal": signal, "gate_values": gate_values, "skip_gain": skip_gain, "filter_spectrum": filter_spectrum}


def tables(length):
    indices = lax.iota(jnp.int32, length)
    angles = 2.0 * math.pi / length * (indices[:, None] * indices[None, :] % length).astype(jnp.float32)
    return (jnp.cos(angles).astype(jnp.bfloat16), jnp.sin(angles).astype(jnp.bfloat16))

def twiddle(c_values, b_values, length):
    angles = 2.0 * math.pi / length * (c_values[:, None] * b_values[None, :] % length).astype(jnp.float32)
    return (jnp.cos(angles), jnp.sin(angles))

def convolve(operands):
    pieces, filter_cols = operands
    cos_a, sin_a = tables(OUTER)
    cos_b, sin_b = tables(INNER)
    inner_table = jnp.stack([cos_b, sin_b]).astype(jnp.float32)
    tw_cos, tw_sin = twiddle(lax.iota(jnp.int32, OUTER), lax.iota(jnp.int32, INNER), SEQ)
    tw_cos = tw_cos[:, :, None]
    tw_sin = tw_sin[:, :, None]
    outer_scale = 1.0 / math.sqrt(OUTER)
    inner_scale = 1.0 / math.sqrt(INNER)
    breadth = pieces.shape[2]
    flattened = pieces.reshape(OUTER, INNER * breadth)
    fwd_re = jnp.dot(cos_a, flattened, preferred_element_type=jnp.float32).reshape(OUTER, INNER, breadth)
    fwd_im = -jnp.dot(sin_a, flattened, preferred_element_type=jnp.float32).reshape(OUTER, INNER, breadth)
    twisted = jnp.stack([(fwd_re * tw_cos + fwd_im * tw_sin) * outer_scale, (fwd_im * tw_cos - fwd_re * tw_sin) * outer_scale]).astype(jnp.bfloat16)
    partials = jnp.einsum('tdb,scbk->tscdk', inner_table, twisted.astype(jnp.float32), precision=lax.Precision.HIGHEST)
    spectrum = jnp.stack([(partials[0, 0] + partials[1, 1]) * inner_scale, (partials[0, 1] - partials[1, 0]) * inner_scale]).astype(jnp.bfloat16)
    filter_re = jnp.swapaxes(filter_cols[0], 0, 1).astype(jnp.float32)
    filter_im = jnp.swapaxes(filter_cols[1], 0, 1).astype(jnp.float32)
    spec_re = spectrum[0].astype(jnp.float32)
    spec_im = spectrum[1].astype(jnp.float32)
    product = jnp.stack([spec_re * filter_re - spec_im * filter_im, spec_re * filter_im + spec_im * filter_re]).astype(jnp.bfloat16)
    partials = jnp.einsum('tbd,scdk->tscbk', inner_table, product.astype(jnp.float32), precision=lax.Precision.HIGHEST)
    back_re = (partials[0, 0] - partials[1, 1]) * inner_scale
    back_im = (partials[0, 1] + partials[1, 0]) * inner_scale
    rotated_re = (back_re * tw_cos - back_im * tw_sin).astype(jnp.bfloat16)
    rotated_im = (back_re * tw_sin + back_im * tw_cos).astype(jnp.bfloat16)
    convolved = (jnp.dot(cos_a, rotated_re.reshape(OUTER, INNER * breadth), preferred_element_type=jnp.float32) - jnp.dot(sin_a, rotated_im.reshape(OUTER, INNER * breadth), preferred_element_type=jnp.float32)) * outer_scale
    return convolved.reshape(OUTER, INNER, breadth).astype(jnp.bfloat16)

def reference(signal, gate_values, skip_gain, filter_spectrum):
    channels = signal.shape[1]
    group_width = 16 if channels % 16 == 0 else channels
    groups = channels // group_width
    signal_grid = signal.reshape(OUTER, INNER, groups, group_width).transpose(2, 0, 1, 3)
    filter_grid = filter_spectrum.reshape(2, INNER, OUTER, groups, group_width).transpose(3, 0, 1, 2, 4)
    convolved = lax.map(convolve, (signal_grid, filter_grid))
    convolved = convolved.transpose(1, 2, 0, 3).reshape(SEQ, channels)
    result = gate_values.astype(jnp.float32) * (convolved.astype(jnp.float32) + skip_gain[None, :].astype(jnp.float32) * signal.astype(jnp.float32))
    return result.astype(jnp.bfloat16)
```

```python
import functools
import math

import jax
import jax.numpy as jnp
from jax import lax
from jax.experimental import pallas as pl
from jax.experimental.pallas import tpu as pltpu
from jax.sharding import PartitionSpec as P


CHUNKS = 2
LANES = 128
NT = (((1,), (1,)), ((), ()))
TN = (((0,), (0,)), ((), ()))
VMEM = 60 * 1024 * 1024


def angles(rows, cols, length):
    return 2.0 * math.pi / length * (rows[:, None] * cols[None, :] % length).astype(jnp.float32)


def make_tables(outer, inner, half, d_rows, zero):
    i_out = lax.iota(jnp.int32, outer) + zero
    i_in = lax.iota(jnp.int32, inner) + zero
    ang = angles(i_out, i_out, outer)
    ta = jnp.concatenate([jnp.cos(ang), jnp.sin(ang)], axis=1).astype(jnp.bfloat16)
    ang = angles(d_rows, i_in, inner)
    cb, sb = jnp.cos(ang).astype(jnp.bfloat16), jnp.sin(ang).astype(jnp.bfloat16)
    g = jnp.concatenate(
        [jnp.concatenate([cb, sb], axis=1), jnp.concatenate([-sb, cb], axis=1)], axis=0
    )
    gi = g.T
    length = outer * inner
    ang = angles(i_out, i_in, length)
    scale = 1.0 / math.sqrt(outer)
    wc, ws = jnp.cos(ang) * scale, jnp.sin(ang) * scale
    ang = angles(i_in, i_out, length)
    scale = 2.0 / math.sqrt(inner)
    vc, vs = jnp.cos(ang) * scale, jnp.sin(ang) * scale
    alt = jnp.where((half == 0) & (i_in % 2 == 1), -1.0, 1.0).astype(jnp.float32)
    row_sign = jnp.broadcast_to(alt[None, :], (8, inner))
    col_sign = jnp.broadcast_to(alt[:, None], (inner, LANES))
    return ta, g, gi, wc, ws, vc, vs, row_sign, col_sign


def conv_kernel(spot_ref, x_ref, *refs, n_h, block):
    h_refs = refs[:n_h]
    ta_ref, g_ref, gi_ref, wc_ref, ws_ref, vc_ref, vs_ref, rs_ref, cs_ref = refs[n_h : n_h + 9]
    o_ref, f_ref, xs_ref, r_ref = refs[n_h + 9 :]
    outer, inner = wc_ref.shape
    half = inner // 2
    f32, b16 = jnp.float32, jnp.bfloat16
    n_src, rows_src, _ = x_ref.shape
    n_ch = pl.num_programs(0)
    ch = pl.program_id(0)
    cc = n_src * rows_src // outer
    tiles = inner // LANES
    inner_scale = 1.0 / math.sqrt(inner)

    @pl.when(ch == 0)
    def _():
        def spread(s, carry):
            v = x_ref[s].astype(f32)
            for t in range(tiles):
                f_ref[t, pl.ds(pl.multiple_of(s * rows_src, rows_src), rows_src), :] = v[
                    :, t * LANES : (t + 1) * LANES
                ]
            return carry

        lax.fori_loop(0, n_src, spread, 0)

    def pick(j, carry):
        for t in range(tiles):
            v = f_ref[t, pl.ds(ch + j * (block * cc), block, stride=cc), :]
            xs_ref[pl.ds(pl.multiple_of(j * block, block), block), t * LANES : (t + 1) * LANES] = (
                v.astype(b16)
            )
        return carry

    lax.fori_loop(0, outer // block, pick, 0)

    def step(i, carry):
        at = pl.multiple_of(i * block, block)
        rows = pl.ds(at, block)
        x = xs_ref[...]
        f_c = jnp.dot(ta_ref[rows, :outer], x, preferred_element_type=f32)
        f_s = jnp.dot(ta_ref[rows, outer:], x, preferred_element_type=f32)
        wc, ws = wc_ref[rows, :], ws_ref[rows, :]
        q_re = (f_c * wc - f_s * ws).astype(b16)
        q_im = (-(f_s * wc + f_c * ws)).astype(b16)
        q = jnp.concatenate([q_re, q_im], axis=1)
        s = lax.dot_general(g_ref[...], q, NT, preferred_element_type=f32) * inner_scale
        s_re = s[:half].astype(b16).astype(f32)
        s_im = s[half:].astype(b16).astype(f32)
        first = (
            (lax.broadcasted_iota(jnp.int32, (half, block), 0) == spot_ref[0])
            & (lax.broadcasted_iota(jnp.int32, (half, block), 1) == 0)
            & (i == 0)
        )
        h_re = jnp.concatenate([h[0, 0, :, rows] for h in h_refs], axis=0).astype(f32)
        h_im = jnp.concatenate([h[0, 1, :, rows] for h in h_refs], axis=0).astype(f32)
        other = jnp.sum(jnp.where(first, h_im, 0.0)[:, :LANES])
        h_re = jnp.where(first, 0.5 * h_re, h_re)
        h_im = jnp.where(first, 0.0, h_im)
        p = jnp.concatenate(
            [(s_re * h_re - s_im * h_im).astype(b16), (s_re * h_im + s_im * h_re).astype(b16)],
            axis=0,
        )
        u = jnp.dot(gi_ref[...], p, preferred_element_type=f32)
        lone = jnp.sum(q_re[:8, :].astype(f32)[:1, :] * rs_ref[:1, :], axis=1, keepdims=True)
        lone = (lone * inner_scale).astype(b16).astype(f32)
        lone = (lone * other).astype(b16).astype(f32) * 0.5
        fix = jnp.where(
            lax.broadcasted_iota(jnp.int32, (inner, LANES), 1) == 0, cs_ref[...] * lone, 0.0
        )
        fix = jnp.concatenate([fix, jnp.zeros((inner, block - LANES), f32)], axis=1)
        u_re = u[:inner] + fix
        u_im = u[inner:]
        vc, vs = vc_ref[:, rows], vs_ref[:, rows]
        r_ref[:, rows] = (u_re * vc - u_im * vs).astype(b16)
        r_ref[:, pl.ds(pl.multiple_of(outer + at, block), block)] = (
            -(u_re * vs + u_im * vc)
        ).astype(b16)
        return carry

    lax.fori_loop(0, outer // block, step, 0)
    outer_scale = 1.0 / math.sqrt(outer)

    def last(j, carry):
        at = pl.multiple_of(j * block, block)
        y = lax.dot_general(
            ta_ref[pl.ds(at, block), :], r_ref[...], NT, preferred_element_type=f32
        )
        y = y * outer_scale
        for t in range(tiles):
            f_ref[t, pl.ds(ch + j * (block * cc), block, stride=cc), :] = y[
                :, t * LANES : (t + 1) * LANES
            ]
        return carry

    lax.fori_loop(0, outer // block, last, 0)

    @pl.when(ch == n_ch - 1)
    def _():
        def collect(s, carry):
            for t in range(tiles):
                v = f_ref[t, pl.ds(pl.multiple_of(s * rows_src, rows_src), rows_src), :]
                o_ref[s, :, t * LANES : (t + 1) * LANES] = v.astype(b16)
            return carry

        lax.fori_loop(0, n_src, collect, 0)


def convolve(spot, x, hs, tables, block=256):
    n_src, rows_src, inner = x.shape
    outer = tables[0].shape[0]
    cc = n_src * rows_src // outer
    const = lambda t: pl.BlockSpec(t.shape, lambda i: (0,) * t.ndim, pipeline_mode=pl.Buffered(1))
    flops = 2 * cc * outer * outer * inner * 6
    return pl.pallas_call(
        functools.partial(conv_kernel, n_h=len(hs), block=block),
        grid=(cc,),
        in_specs=[
            pl.BlockSpec(memory_space=pltpu.SMEM),
            const(x),
            *[pl.BlockSpec((1,) + h.shape[1:], lambda i: (i, 0, 0, 0)) for h in hs],
            *[const(t) for t in tables],
        ],
        out_specs=const(x),
        out_shape=jax.ShapeDtypeStruct(x.shape, jnp.bfloat16),
        scratch_shapes=[
            pltpu.VMEM((inner // LANES, outer * cc, LANES), jnp.float32),
            pltpu.VMEM((outer, inner), jnp.bfloat16),
            pltpu.VMEM((inner, 2 * outer), jnp.bfloat16),
        ],
        compiler_params=pltpu.CompilerParams(vmem_limit_bytes=VMEM),
        cost_estimate=pl.CostEstimate(
            flops=flops, bytes_accessed=2 * (2 * x.size + 8 * hs[0].size), transcendentals=0
        ),
        name="convolve",
    )(spot, x, *hs, *tables)


def order(shards, ch_dev, chunks, ap):
    cc = ch_dev // chunks
    r = lax.iota(jnp.int32, chunks * shards * ap * cc)
    c = r % cc
    a = r // cc % ap
    dest = r // (cc * ap) % shards
    k = r // (cc * ap * shards)
    return a * (shards * ch_dev) + dest * ch_dev + k * cc + c


def split_kernel(sel_ref, x_ref, *o_refs, ap):
    a_blk, inner, _ = x_ref.shape
    rows = sel_ref.shape[0] // len(o_refs)

    def step(g, carry):
        x = jnp.concatenate([x_ref[g * ap + j] for j in range(ap)], axis=1)
        y = lax.dot_general(sel_ref[...], x, NT, preferred_element_type=jnp.float32)
        y = y.astype(jnp.bfloat16)
        for k, o_ref in enumerate(o_refs):
            n_dest = o_ref.shape[0]
            per = rows // n_dest
            o_ref[:, pl.ds(pl.multiple_of(g * per, per), per), :] = y[
                k * rows : (k + 1) * rows
            ].reshape(n_dest, per, inner)
        return carry

    lax.fori_loop(0, a_blk // ap, step, 0)


def split_signal(signal, shards, chunks):
    a_loc, inner, channels = signal.shape
    ch_dev = channels // shards
    cc = ch_dev // chunks
    ap = max(1, 8 // cc)
    a_blk = min(a_loc, max(8, 16 // cc, ap))
    cols = order(shards, ch_dev, chunks, ap)
    sel = (cols[:, None] == lax.iota(jnp.int32, ap * channels)[None, :]).astype(jnp.bfloat16)
    out = jax.ShapeDtypeStruct((shards, a_loc * cc, inner), jnp.bfloat16)
    return pl.pallas_call(
        functools.partial(split_kernel, ap=ap),
        grid=(a_loc // a_blk,),
        in_specs=[
            pl.BlockSpec(sel.shape, lambda i: (0, 0)),
            pl.BlockSpec((a_blk, inner, channels), lambda i: (i, 0, 0)),
        ],
        out_specs=[pl.BlockSpec((shards, a_blk * cc, inner), lambda i: (0, i, 0))] * chunks,
        out_shape=[out] * chunks,
        compiler_params=pltpu.CompilerParams(vmem_limit_bytes=VMEM),
        cost_estimate=pl.CostEstimate(
            flops=2 * signal.size * sel.shape[0], bytes_accessed=4 * signal.size, transcendentals=0
        ),
        name="split_signal",
    )(sel, signal)


def merge_kernel(sel_ref, skip_ref, sig_ref, gate_ref, *refs, ap):
    y_refs, o_ref = refs[:-1], refs[-1]
    a_blk, inner, channels = sig_ref.shape
    f32 = jnp.float32

    def step(g, carry):
        parts = []
        for y_ref in y_refs:
            n_src, rows_blk, _ = y_ref.shape
            per = rows_blk * ap // a_blk
            y = y_ref[:, pl.ds(pl.multiple_of(g * per, per), per), :]
            parts.append(y.reshape(n_src * per, inner))
        y = jnp.concatenate(parts, axis=0)
        z = lax.dot_general(y, sel_ref[...], TN, preferred_element_type=f32)
        for j in range(ap):
            at = g * ap + j
            conv = z[:, j * channels : (j + 1) * channels]
            total = conv + skip_ref[...] * sig_ref[at].astype(f32)
            o_ref[at] = (gate_ref[at].astype(f32) * total).astype(o_ref.dtype)
        return carry

    lax.fori_loop(0, a_blk // ap, step, 0)


def merge(ys, signal, gate, skip, shards):
    a_loc, inner, channels = signal.shape
    chunks = len(ys)
    ch_dev = channels // shards
    cc = ch_dev // chunks
    ap = max(1, 8 // cc)
    a_blk = min(a_loc, max(8, 16 // cc, ap))
    cols = order(shards, ch_dev, chunks, ap)
    sel = (cols[:, None] == lax.iota(jnp.int32, ap * channels)[None, :]).astype(jnp.bfloat16)
    whole = pl.BlockSpec((a_blk, inner, channels), lambda i: (i, 0, 0))
    return pl.pallas_call(
        functools.partial(merge_kernel, ap=ap),
        grid=(a_loc // a_blk,),
        in_specs=[
            pl.BlockSpec(sel.shape, lambda i: (0, 0)),
            pl.BlockSpec((1, channels), lambda i: (0, 0)),
            whole,
            whole,
            *[pl.BlockSpec((shards, a_blk * cc, inner), lambda i: (0, i, 0))] * chunks,
        ],
        out_specs=whole,
        out_shape=jax.ShapeDtypeStruct(signal.shape, jnp.bfloat16),
        compiler_params=pltpu.CompilerParams(vmem_limit_bytes=VMEM),
        cost_estimate=pl.CostEstimate(
            flops=2 * signal.size * sel.shape[0], bytes_accessed=8 * signal.size, transcendentals=0
        ),
        name="merge",
    )(sel, skip, signal, gate, *ys)


def exchange(v):
    return lax.all_to_all(v, "seq", split_axis=0, concat_axis=0, tiled=True)


def layer(signal, gate_values, skip_gain, filter_spectrum):
    shards = lax.axis_size("seq")
    me = lax.axis_index("seq")
    positions, channels = signal.shape
    _, d_loc, outer, _ = filter_spectrum.shape
    inner = d_loc * shards
    a_loc = positions // inner
    ch_dev = channels // shards
    chunks = CHUNKS
    cc = ch_dev // chunks
    group = shards // 2
    half = me // group
    mine = me % group
    zero = me // shards
    barrier = lax.optimization_barrier

    row = lax.ppermute(filter_spectrum[0, 0, 0, :], "seq", [(0, group), (group, 0)])

    signal = signal.reshape(a_loc, inner, channels)
    xs = list(split_signal(signal, shards, chunks))
    xs[0], row = barrier((xs[0], row))
    got = [None] * chunks
    got[0] = exchange(xs[0])

    filt = filter_spectrum.transpose(3, 0, 1, 2)
    spot_im = jnp.where(mine == 0, row, filt[:, 1, 0, 0])
    filt = filt.at[:, 1, 0, 0].set(spot_im)
    filt = filt.reshape(2, group, chunks, cc, 2, d_loc, outer)
    cut = [
        [filt[half, (mine + s) % group, k] for s in range(group)] for k in range(chunks)
    ]
    hs = []
    for k in range(chunks):
        pieces = []
        for s, piece in enumerate(cut[k]):
            if s:
                pairs = [
                    (b * group + i, b * group + (i + s) % group)
                    for b in range(2)
                    for i in range(group)
                ]
                piece = lax.ppermute(piece, "seq", pairs)
            pieces.append(piece)
        hs.append(pieces)

    shift = lax.iota(jnp.int32, group)
    src = (mine - shift) % group
    d_rows = (half * group + src)[:, None] * d_loc + lax.iota(jnp.int32, d_loc)[None, :]
    tables = make_tables(outer, inner, half, d_rows.reshape(-1), zero)
    spot = (mine * d_loc).reshape(1)

    for k in range(1, chunks):
        extra = (tables, cut) if k == 1 else ()
        xs[k], got[k - 1], extra = barrier((xs[k], got[k - 1], extra))
        if k == 1:
            tables = extra[0]
        got[k] = exchange(xs[k])
    ys = []
    for k in range(chunks):
        out = convolve(spot, got[k], hs[k], tables)
        if k + 1 < chunks:
            out, hs[k + 1] = barrier((out, hs[k + 1]))
        ys.append(exchange(out))
    out = merge(ys, signal, gate_values.reshape(signal.shape), skip_gain[None, :], shards)
    return out.reshape(positions, channels)


def solution(mesh):
    return jax.shard_map(
        layer,
        mesh=mesh,
        in_specs=(P("seq", "chan"), P("seq", "chan"), P("chan"), P(None, "seq", None, "chan")),
        out_specs=P("seq", "chan"),
        check_vma=False,
    )
```

```python
import functools
import math

import jax
import jax.numpy as jnp
from jax import lax
from jax.experimental import pallas as pl
from jax.experimental.pallas import tpu as pltpu
from jax.sharding import PartitionSpec as P


CHUNKS = 2
BLOCK = 128
MOVE = 256
LANES = 128
NT = (((1,), (1,)), ((), ()))
TN = (((0,), (0,)), ((), ()))
VMEM = 60 * 1024 * 1024


def angles(rows, cols, length):
    return 2.0 * math.pi / length * (rows[:, None] * cols[None, :] % length).astype(jnp.float32)


def make_tables(outer, inner, half, d_rows, zero):
    b16 = jnp.bfloat16
    side = lambda ang: jnp.concatenate([jnp.cos(ang), jnp.sin(ang)], axis=1).astype(b16)
    i_out = lax.iota(jnp.int32, outer) + zero
    i_in = lax.iota(jnp.int32, inner) + zero
    low = lax.iota(jnp.int32, outer // 2) + zero
    even = side(angles(low, 2 * low, outer))
    odd = side(angles(low, 2 * low + 1, outer))
    odd_t = side(angles(2 * low + 1, low, outer))
    ang = angles(i_in, d_rows, inner)
    cb, sb = jnp.cos(ang).astype(b16), jnp.sin(ang).astype(b16)
    g = jnp.concatenate(
        [jnp.concatenate([cb, -sb], axis=1), jnp.concatenate([sb, cb], axis=1)], axis=0
    )
    ang = angles(d_rows, i_in, inner)
    cb, sb = jnp.cos(ang).astype(b16), jnp.sin(ang).astype(b16)
    gi = jnp.concatenate(
        [jnp.concatenate([cb, sb], axis=1), jnp.concatenate([-sb, cb], axis=1)], axis=0
    )
    ang = angles(i_out, i_in, outer * inner)
    scale = 1.0 / math.sqrt(outer)
    wc, ws = jnp.cos(ang) * scale, jnp.sin(ang) * scale
    alt = jnp.where((half == 0) & (i_in % 2 == 1), -1.0, 1.0).astype(jnp.float32)
    return even, odd, odd_t, g, gi, wc, ws, jnp.broadcast_to(alt[None, :], (8, inner))


def spread(x_refs, f_ref, me, n_src):
    tiles, total, _ = f_ref.shape
    per = total // n_src

    def one(x_ref, s, at):
        v = x_ref[s].astype(jnp.float32)
        rows = pl.ds(pl.multiple_of(at * per, per), per)
        for t in range(tiles):
            f_ref[t, rows, :] = v[:, t * LANES : (t + 1) * LANES]
        return 0

    if len(x_refs) == 1:
        lax.fori_loop(0, n_src, lambda s, carry: one(x_refs[0], s, s), 0)
    else:
        for s, x_ref in enumerate(x_refs):
            one(x_ref, 0, me ^ s)


def collect(f_ref, o_refs, me, n_src):
    tiles, total, _ = f_ref.shape
    per = total // n_src

    def one(o_ref, s, at):
        rows = pl.ds(pl.multiple_of(at * per, per), per)
        for t in range(tiles):
            o_ref[s, :, t * LANES : (t + 1) * LANES] = f_ref[t, rows, :].astype(o_ref.dtype)
        return 0

    if len(o_refs) == 1:
        lax.fori_loop(0, n_src, lambda s, carry: one(o_refs[0], s, s), 0)
    else:
        for s, o_ref in enumerate(o_refs):
            one(o_ref, 0, me ^ s)


def forward_kernel(spot_ref, *refs, n_x, block):
    x_refs, refs = refs[:n_x], refs[n_x:]
    te_ref, to_ref, g_ref, wc_ref, ws_ref, sg_ref, s_ref, l_ref, f_ref, xe_ref, xo_ref = refs
    outer, inner = wc_ref.shape
    low = outer // 2
    f32, b16 = jnp.float32, jnp.bfloat16
    ch = pl.program_id(0)
    tiles, total, _ = f_ref.shape
    cc = total // outer
    n_src = total // x_refs[0].shape[-2]
    inner_scale = 1.0 / math.sqrt(inner)

    @pl.when(ch == 0)
    def _():
        spread(x_refs, f_ref, spot_ref[1], n_src)

    def pick(j, carry):
        rows = pl.ds(pl.multiple_of(j * MOVE, MOVE), MOVE)
        for odd, ref in enumerate((xe_ref, xo_ref)):
            for t in range(tiles):
                v = f_ref[t, pl.ds(ch + odd * cc + j * (2 * MOVE * cc), MOVE, stride=2 * cc), :]
                ref[rows, t * LANES : (t + 1) * LANES] = v.astype(b16)
        return carry

    lax.fori_loop(0, low // MOVE, pick, 0)

    def step(i, carry):
        at = pl.multiple_of(i * block, block)
        rows = pl.ds(at, block)
        high = pl.ds(pl.multiple_of(low + at, block), block)
        dot = functools.partial(jnp.dot, preferred_element_type=f32)
        xe, xo = xe_ref[...], xo_ref[...]
        e_c, o_c = dot(te_ref[rows, :low], xe), dot(to_ref[rows, :low], xo)
        e_s, o_s = dot(te_ref[rows, low:], xe), dot(to_ref[rows, low:], xo)
        parts = []
        for f_c, f_s, at_w in ((e_c + o_c, e_s + o_s, rows), (e_c - o_c, e_s - o_s, high)):
            wc, ws = wc_ref[at_w, :], ws_ref[at_w, :]
            q_re = (f_c * wc - f_s * ws).astype(b16)
            q_im = (-(f_s * wc + f_c * ws)).astype(b16)
            parts.append(jnp.concatenate([q_re, q_im], axis=1))
        q = jnp.concatenate(parts, axis=0)
        s = (dot(q, g_ref[...]) * inner_scale).astype(b16)
        s_ref[0, rows, :] = s[:block]
        s_ref[0, high, :] = s[block:]

        @pl.when(i == 0)
        def _():
            lone = jnp.sum(q[:8, :inner].astype(f32)[:1] * sg_ref[:1, :], axis=1, keepdims=True)
            lone = (lone * inner_scale).astype(b16).astype(f32)
            l_ref[0] = jnp.broadcast_to(lone, l_ref.shape[1:])

        return carry

    lax.fori_loop(0, low // block, step, 0)


def inverse_kernel(spot_ref, s_ref, l_ref, *refs, n_x, n_h, block):
    h_refs, refs = refs[:n_h], refs[n_h:]
    te_ref, tt_ref, gi_ref, wc_ref, ws_ref, sg_ref = refs[:6]
    o_refs, (f_ref, rp_ref, rm_ref) = refs[6 : 6 + n_x], refs[6 + n_x :]
    outer, inner = wc_ref.shape
    low, half = outer // 2, inner // 2
    f32, b16 = jnp.float32, jnp.bfloat16
    ch = pl.program_id(0)
    n_ch = pl.num_programs(0)
    tiles, total, _ = f_ref.shape
    cc = total // outer
    n_src = total // o_refs[0].shape[-2]

    def step(i, carry):
        at = pl.multiple_of(i * block, block)
        rows = pl.ds(at, block)
        high = pl.ds(pl.multiple_of(low + at, block), block)
        s = jnp.concatenate([s_ref[0, rows, :], s_ref[0, high, :]], axis=0)
        s_re, s_im = s[:, :half].astype(f32), s[:, half:].astype(f32)
        h_re, h_im = (
            jnp.concatenate(
                [
                    jnp.concatenate([r[0, p, :, at_h] for r in h_refs], axis=0).T
                    for at_h in (rows, high)
                ],
                axis=0,
            ).astype(f32)
            for p in range(2)
        )
        top = lax.broadcasted_iota(jnp.int32, (8, half), 0) == 0
        first = top & (lax.broadcasted_iota(jnp.int32, (8, half), 1) == spot_ref[0]) & (i == 0)
        other = jnp.sum(jnp.where(first, h_im[:8], 0.0))
        h_re = jnp.concatenate([jnp.where(first, 0.5 * h_re[:8], h_re[:8]), h_re[8:]], axis=0)
        h_im = jnp.concatenate([jnp.where(first, 0.0, h_im[:8]), h_im[8:]], axis=0)
        p = jnp.concatenate(
            [(s_re * h_re - s_im * h_im).astype(b16), (s_re * h_im + s_im * h_re).astype(b16)],
            axis=1,
        )
        u = jnp.dot(p, gi_ref[...], preferred_element_type=f32)
        lone = (l_ref[0, :1, :1] * other).astype(b16).astype(f32) * 0.5
        u_re, u_im = u[:, :inner], u[:, inner:]
        fix = jnp.where(lax.broadcasted_iota(jnp.int32, (8, inner), 0) == 0, sg_ref[...] * lone, 0.0)
        u_re = jnp.concatenate([u_re[:8] + fix, u_re[8:]], axis=0)
        r = []
        for k, at_w in enumerate((rows, high)):
            a_re, a_im = u_re[k * block : (k + 1) * block], u_im[k * block : (k + 1) * block]
            wc, ws = wc_ref[at_w, :], ws_ref[at_w, :]
            r.append((a_re * wc - a_im * ws, -(a_re * ws + a_im * wc)))
        for part, at_r in enumerate((rows, high)):
            rp_ref[at_r, :] = (r[0][part] + r[1][part]).astype(b16)
            rm_ref[at_r, :] = (r[0][part] - r[1][part]).astype(b16)
        return carry

    lax.fori_loop(0, low // block, step, 0)
    scale = 2.0 / math.sqrt(inner)

    def last(j, carry):
        rows = pl.ds(pl.multiple_of(j * MOVE, MOVE), MOVE)
        for odd, (t_ref, r_ref) in enumerate(((te_ref, rp_ref), (tt_ref, rm_ref))):
            y = jnp.dot(t_ref[rows, :], r_ref[...], preferred_element_type=f32) * scale
            for t in range(tiles):
                f_ref[t, pl.ds(ch + odd * cc + j * (2 * MOVE * cc), MOVE, stride=2 * cc), :] = y[
                    :, t * LANES : (t + 1) * LANES
                ]
        return carry

    lax.fori_loop(0, low // MOVE, last, 0)

    @pl.when(ch == n_ch - 1)
    def _():
        collect(f_ref, o_refs, spot_ref[1], n_src)


def whole_spec(t):
    return pl.BlockSpec(t.shape, lambda i: (0,) * t.ndim, pipeline_mode=pl.Buffered(1))


def channel_spec(t):
    return pl.BlockSpec((1,) + t.shape[1:], lambda i: (i,) + (0,) * (t.ndim - 1))


def forward(spot, xs, tables, block=BLOCK):
    te, to, _, g, _, wc, ws, sg = tables
    outer, inner = wc.shape
    size = sum(x.size for x in xs)
    cc = size // (outer * inner)
    out = jax.ShapeDtypeStruct((cc, outer, inner), jnp.bfloat16)
    lone = jax.ShapeDtypeStruct((cc, 8, LANES), jnp.float32)
    consts = (te, to, g, wc, ws, sg)
    return pl.pallas_call(
        functools.partial(forward_kernel, n_x=len(xs), block=block),
        grid=(cc,),
        in_specs=[pl.BlockSpec(memory_space=pltpu.SMEM), *[whole_spec(t) for t in (*xs, *consts)]],
        out_specs=[channel_spec(out), channel_spec(lone)],
        out_shape=[out, lone],
        scratch_shapes=[
            pltpu.VMEM((inner // LANES, outer * cc, LANES), jnp.float32),
            *[pltpu.VMEM((outer // 2, inner), jnp.bfloat16)] * 2,
        ],
        compiler_params=pltpu.CompilerParams(vmem_limit_bytes=VMEM),
        cost_estimate=pl.CostEstimate(
            flops=2 * cc * outer * outer * inner * 2, bytes_accessed=4 * size, transcendentals=0
        ),
        name="forward",
    )(spot, *xs, *consts)


def inverse(spot, spectrum, lone, hs, shards, count, tables, block=BLOCK):
    te, _, tt, _, gi, wc, ws, sg = tables
    outer, inner = wc.shape
    cc = spectrum.shape[0]
    consts = (te, tt, gi, wc, ws, sg)
    shape = (shards // count, outer // shards * cc, inner)
    outs = [jax.ShapeDtypeStruct(shape, jnp.bfloat16)] * count
    size = 2 * spectrum.size + len(hs) * hs[0].size
    return pl.pallas_call(
        functools.partial(inverse_kernel, n_x=count, n_h=len(hs), block=block),
        grid=(cc,),
        in_specs=[
            pl.BlockSpec(memory_space=pltpu.SMEM),
            *[channel_spec(t) for t in (spectrum, lone, *hs)],
            *[whole_spec(t) for t in consts],
        ],
        out_specs=[whole_spec(x) for x in outs],
        out_shape=outs,
        scratch_shapes=[
            pltpu.VMEM((inner // LANES, outer * cc, LANES), jnp.float32),
            *[pltpu.VMEM((outer, inner), jnp.bfloat16)] * 2,
        ],
        compiler_params=pltpu.CompilerParams(vmem_limit_bytes=VMEM),
        cost_estimate=pl.CostEstimate(
            flops=2 * cc * outer * outer * inner * 2, bytes_accessed=2 * size, transcendentals=0
        ),
        name="inverse",
    )(spot, spectrum, lone, *hs, *consts)


def order(me, shards, ch_dev, chunks, ap, swapped):
    cc = ch_dev // chunks
    r = lax.iota(jnp.int32, chunks * shards * ap * cc)
    c = r % cc
    a = r // cc % ap
    piece = r // (cc * ap) % shards
    k = r // (cc * ap * shards)
    piece = jnp.where(k % 2 == swapped, me ^ piece, piece)
    cols = a * (shards * ch_dev) + piece * ch_dev + k * cc + c
    return (cols[:, None] == lax.iota(jnp.int32, ap * shards * ch_dev)[None, :]).astype(jnp.bfloat16)


def pieces_of(shards, k, swapped):
    return shards if k % 2 == swapped else 1


def split_kernel(sel_ref, x_ref, *o_refs, ap, chunks, shards):
    a_blk, inner, _ = x_ref.shape
    rows = sel_ref.shape[0] // chunks
    per = rows // shards

    def step(g, carry):
        x = jnp.concatenate([x_ref[g * ap + j] for j in range(ap)], axis=1)
        y = lax.dot_general(sel_ref[...], x, NT, preferred_element_type=jnp.float32)
        y = y.astype(jnp.bfloat16).reshape(chunks, shards, per, inner)
        at = pl.ds(pl.multiple_of(g * per, per), per)
        n = 0
        for k in range(chunks):
            count = pieces_of(shards, k, 1)
            for s in range(count):
                o_refs[n][:, at, :] = y[k] if count == 1 else y[k, s : s + 1]
                n += 1
        return carry

    lax.fori_loop(0, a_blk // ap, step, 0)


def blocks(a_loc, cc):
    ap = max(1, 16 // cc)
    return ap, min(a_loc, max(16, ap))


def piece_specs(shards, chunks, rows, inner, swapped):
    return [
        pl.BlockSpec((shards // pieces_of(shards, k, swapped), rows, inner), lambda i: (0, i, 0))
        for k in range(chunks)
        for _ in range(pieces_of(shards, k, swapped))
    ]


def split_signal(me, signal, shards, chunks):
    a_loc, inner, channels = signal.shape
    ch_dev = channels // shards
    cc = ch_dev // chunks
    ap, a_blk = blocks(a_loc, cc)
    sel = order(me, shards, ch_dev, chunks, ap, 1)
    specs = piece_specs(shards, chunks, a_blk * cc, inner, 1)
    outs = pl.pallas_call(
        functools.partial(split_kernel, ap=ap, chunks=chunks, shards=shards),
        grid=(a_loc // a_blk,),
        in_specs=[
            pl.BlockSpec(sel.shape, lambda i: (0, 0)),
            pl.BlockSpec((a_blk, inner, channels), lambda i: (i, 0, 0)),
        ],
        out_specs=specs,
        out_shape=[
            jax.ShapeDtypeStruct((s.block_shape[0], a_loc * cc, inner), jnp.bfloat16) for s in specs
        ],
        compiler_params=pltpu.CompilerParams(vmem_limit_bytes=VMEM),
        cost_estimate=pl.CostEstimate(
            flops=2 * signal.size * sel.shape[0], bytes_accessed=4 * signal.size, transcendentals=0
        ),
        name="split_signal",
    )(sel, signal)
    return by_chunk(outs, shards, chunks)


def by_chunk(pieces, shards, chunks):
    out, n = [], 0
    for k in range(chunks):
        count = pieces_of(shards, k, 1)
        out.append(list(pieces[n : n + count]))
        n += count
    return out


def merge_kernel(sel_ref, skip_ref, sig_ref, gate_ref, *refs, ap):
    y_refs, o_ref = refs[:-1], refs[-1]
    a_blk, inner, channels = sig_ref.shape
    f32 = jnp.float32

    def step(g, carry):
        parts = []
        for y_ref in y_refs:
            n_src, rows_blk, _ = y_ref.shape
            per = rows_blk * ap // a_blk
            y = y_ref[:, pl.ds(pl.multiple_of(g * per, per), per), :]
            parts.append(y.reshape(n_src * per, inner))
        y = jnp.concatenate(parts, axis=0)
        z = lax.dot_general(y, sel_ref[...], TN, preferred_element_type=f32)
        for j in range(ap):
            at = g * ap + j
            conv = z[:, j * channels : (j + 1) * channels]
            total = conv + skip_ref[...] * sig_ref[at].astype(f32)
            o_ref[at] = (gate_ref[at].astype(f32) * total).astype(o_ref.dtype)
        return carry

    lax.fori_loop(0, a_blk // ap, step, 0)


def merge(me, ys, signal, gate, skip, shards):
    a_loc, inner, channels = signal.shape
    chunks = len(ys)
    ch_dev = channels // shards
    cc = ch_dev // chunks
    ap, a_blk = blocks(a_loc, cc)
    sel = order(me, shards, ch_dev, chunks, ap, 0)
    whole = pl.BlockSpec((a_blk, inner, channels), lambda i: (i, 0, 0))
    return pl.pallas_call(
        functools.partial(merge_kernel, ap=ap),
        grid=(a_loc // a_blk,),
        in_specs=[
            pl.BlockSpec(sel.shape, lambda i: (0, 0)),
            pl.BlockSpec((1, channels), lambda i: (0, 0)),
            whole,
            whole,
            *piece_specs(shards, chunks, a_blk * cc, inner, 0),
        ],
        out_specs=whole,
        out_shape=jax.ShapeDtypeStruct(signal.shape, jnp.bfloat16),
        compiler_params=pltpu.CompilerParams(vmem_limit_bytes=VMEM),
        cost_estimate=pl.CostEstimate(
            flops=2 * signal.size * sel.shape[0], bytes_accessed=8 * signal.size, transcendentals=0
        ),
        name="merge",
    )(sel, skip, signal, gate, *[y for pieces in ys for y in pieces])


def exchange(pieces, shards, far_first=False):
    if len(pieces) == 1:
        return [lax.all_to_all(pieces[0], "seq", split_axis=0, concat_axis=0, tiled=True)]
    return swap(pieces, shards, far_first)


def swap(pieces, shards, far_first=False):
    out, n = list(pieces), len(pieces)
    near, far = range(n // 4, n // 2), range(n // 2, n)
    ranks = (near, far, range(1, n // 4)) if n == shards else (far, range(1, n // 2))
    if far_first:
        ranks = (far, near, range(1, n // 4))
    for members in ranks:
        for s in members:
            out[s] = lax.ppermute(pieces[s], "seq", [(i, i ^ s) for i in range(shards)])
    return out


def layer(signal, gate_values, skip_gain, filter_spectrum):
    shards = lax.axis_size("seq")
    me = lax.axis_index("seq")
    positions, channels = signal.shape
    _, d_loc, outer, _ = filter_spectrum.shape
    inner = d_loc * shards
    a_loc = positions // inner
    ch_dev = channels // shards
    chunks = CHUNKS
    cc = ch_dev // chunks
    group = shards // 2
    half = me // group
    mine = me % group
    zero = me // shards
    barrier = lax.optimization_barrier

    row = lax.ppermute(filter_spectrum[0, 0, 0, :], "seq", [(0, group), (group, 0)])

    signal = signal.reshape(a_loc, inner, channels)
    xs = split_signal(me, signal, shards, chunks)
    xs[0], row = barrier((xs[0], row))
    got = [None] * chunks
    got[0] = exchange(xs[0], shards)

    filt = filter_spectrum.transpose(3, 0, 1, 2)
    spot_im = jnp.where(mine == 0, row, filt[:, 1, 0, 0])
    filt = filt.at[:, 1, 0, 0].set(spot_im)
    filt = filt.reshape(2, group, chunks, cc, 2, d_loc, outer)
    cut = [
        [filt[half, mine ^ s, k] for s in range(group)] for k in range(chunks)
    ]
    hs = []
    for k in range(chunks):
        hs.append(swap(cut[k], shards))

    shift = lax.iota(jnp.int32, group)
    src = mine ^ shift
    d_rows = (half * group + src)[:, None] * d_loc + lax.iota(jnp.int32, d_loc)[None, :]
    tables = make_tables(outer, inner, half, d_rows.reshape(-1), zero)
    spot = jnp.stack([mine * d_loc, me])

    for k in range(1, chunks):
        got[k] = exchange(xs[k], shards)
    ys = []
    for k in range(chunks):
        spectrum = forward(spot, got[k], tables)
        out = inverse(
            spot, *spectrum, hs[k], shards, pieces_of(shards, k, 0), tables
        )
        ys.append(exchange(out, shards, far_first=True))
    out = merge(me, ys, signal, gate_values.reshape(signal.shape), skip_gain[None, :], shards)
    return out.reshape(positions, channels)


def solution(mesh):
    return jax.shard_map(
        layer,
        mesh=mesh,
        in_specs=(P("seq", "chan"), P("seq", "chan"), P("chan"), P(None, "seq", None, "chan")),
        out_specs=P("seq", "chan"),
        check_vma=False,
    )
```
